32 devices in a mesh: row: 8 (over y, x, core), col: 4 (over z).
Axes of the slice: x: 2, y: 2, z: 4, core: 2. Of those that a mesh axis runs over, the one named last changes fastest.
Arguments:
- tokens: bfloat16 [1024, 8192], P('row', 'col'), may hold values from -6 to 6
- weights: bfloat16 [2, 14336, 8192], P(None, 'row', 'col'), may hold values from -0.0625 to 0.0625
- gradients: bfloat16 [2, 14336, 8192], P(None, 'row', 'col'), may hold values from -200 to 200, as said below
- row_factors: float32 [2, 14336], P(None, 'row'), may hold values from 0.05 to 0.5
- col_factors: float32 [2, 8192], P(None, 'col'), may hold values from 0.05 to 0.5
Outputs:
- hidden: bfloat16 [1024, 14336], P('col', 'row')
- row_new: float32 [2, 14336], P(None, 'row')
- col_new: float32 [2, 8192], P(None, 'col')
The draws below stay inside these ranges and needn't reach their ends.
Inputs may be any that keep to these rules, and one draw needn't show every extreme that they name: Finite real gradients.
All inputs are finite; a program needn't handle non-finite values.
Results may differ from the reference program's by a relative error of at most 0.001.
The reference program's roundings to bfloat16 on the way (of `new_weights`) count: a program that leaves them out, or rounds other values in their place, can miss the bound.
Values may be sent and summed in bfloat16 or wider, within the bound.
A program may use at most 128 MiB of HBM per device.

```python
import math
import jax
import jax.numpy as jnp
from jax import lax

D = 8192
FF = 14336
TOKENS = 1024


def draw_gradients(key, part):
    keys = jax.random.split(jax.random.fold_in(key, 17), 5)
    row_pos = jnp.arange(FF, dtype=jnp.float32) / FF
    col_pos = jnp.arange(D, dtype=jnp.float32) / D
    row_scale = 0.5 * jnp.power(3.0, row_pos)[None, :, None] * jnp.exp(jax.random.uniform(keys[0], (2, FF, 1), jnp.float32, math.log(0.4), math.log(2.5)))
    col_scale = 0.5 * jnp.power(3.0, col_pos)[None, None, :] * jnp.exp(jax.random.uniform(keys[1], (2, 1, D), jnp.float32, math.log(0.4), math.log(2.5)))
    values = jax.random.normal(keys[4], (2, FF, D), jnp.float32) * row_scale * col_scale
    return jnp.clip(values, -200.0, 200.0).astype(jnp.bfloat16)


def block_levels(key, dims, shards, least, largest):
    gain = 1.0
    for dim, parts in shards:
        heights = jax.random.uniform(jax.random.fold_in(jax.random.fold_in(key, 6), dim), (parts,), jnp.float32, least / len(shards), largest / len(shards))
        gain = gain * jnp.repeat(jnp.exp(heights), dims[dim] // parts).reshape((-1,) + (1,) * (len(dims) - 1 - dim))
    return gain


def bell_draw(rng, shape, deviation, limit, cuts=(), kind=jnp.bfloat16):
    gain = block_levels(rng, shape, cuts, -0.22, 0.18) if cuts else 1.0
    values = jax.random.normal(rng, shape, jnp.float32) * deviation * gain
    return jnp.minimum(jnp.maximum(values, -limit), limit).astype(kind)


def setup_inputs(seed: int = 0) -> dict:
    key_list = jax.random.split(jax.random.key(seed), 6)
    return {
        "tokens": bell_draw(key_list[0], (TOKENS, D), 1.0, 6.0, ((0, 8), (1, 4))),
        "weights": bell_draw(key_list[1], (2, FF, D), D ** -0.5, 0.0625, ((1, 8), (2, 4))),
        "gradients": draw_gradients(jax.random.fold_in(key_list[5], 71), 0),
        "row_factors": jnp.clip(jnp.exp(math.log(0.5) - 2.3025851 * jax.random.uniform(key_list[3], (2, FF), jnp.float32) ** block_levels(key_list[3], (2, FF), ((1, 8),), -0.2, 0.2)), 0.05, 0.5),
        "col_factors": jnp.clip(jnp.exp(math.log(0.5) - 2.3025851 * jax.random.uniform(key_list[4], (2, D), jnp.float32) ** block_levels(key_list[4], (2, D), ((1, 4),), -0.2, 0.2)), 0.05, 0.5),
    }


decay_rate = 0.5
learn_rate = 0.01
clip_limit = 1.0
tiny_eps = 1e-30

def reference(tokens, weights, gradients, row_factors, col_factors):
    gradient = gradients.astype(jnp.float32)
    squares = gradient * gradient
    row_new = decay_rate * row_factors + (1.0 - decay_rate) * (lax.optimization_barrier(jnp.mean(squares, axis=2)) + tiny_eps)
    col_new = decay_rate * col_factors + (1.0 - decay_rate) * (lax.optimization_barrier(jnp.mean(squares, axis=1)) + tiny_eps)
    row_mean = lax.optimization_barrier(jnp.mean(row_new, axis=1))
    denominator = jnp.sqrt(row_new[:, :, None] * col_new[:, None, :] / row_mean[:, None, None])
    update = gradient / denominator
    rms_value = jnp.sqrt(lax.optimization_barrier(jnp.mean(update * update, axis=(1, 2))))
    clip_scale = jnp.maximum(1.0, rms_value / clip_limit)
    new_weights = (weights.astype(jnp.float32) - learn_rate * update / clip_scale[:, None, None]).astype(jnp.bfloat16)
    gate_proj = lax.dot_general(tokens, new_weights[0], (((1,), (1,)), ((), ())), preferred_element_type=jnp.float32)
    up_proj = lax.dot_general(tokens, new_weights[1], (((1,), (1,)), ((), ())), preferred_element_type=jnp.float32)
    hidden = (jax.nn.silu(gate_proj) * up_proj).astype(jnp.bfloat16)
    return (hidden, row_new, col_new)
```

```python
import functools
import jax
import jax.numpy as jnp
from jax import lax
from jax.experimental import pallas as pl
from jax.experimental.pallas import tpu as pltpu
from jax.sharding import PartitionSpec as P

decay_rate = 0.5
learn_rate = 0.01
clip_limit = 1.0
tiny_eps = 1e-30
code_span = 250.0


MESH = pl.DeviceIdType.MESH
LANES = 128
STRIP = 32
END_LAG = 8
INNER_LAG = 3


def flip(value, mask):
    return value + mask * (1 - 2 * ((value // mask) % 2))


def subsets(value, masks):
    out = [value]
    for mask in masks:
        out = out + [flip(item, mask) for item in out]
    return out


def body(
    rows,
    cols,
    chunks,
    tok_in,
    w_in,
    g_in,
    rf_ref,
    cf_ref,
    out_ref,
    row_out,
    col_out,
    tok,
    w,
    g,
    rcol,
    colacc,
    cgain,
    rslot,
    cslot,
    s1,
    s2,
    prod,
    sbuf,
    rbuf,
    sscale,
    rscale,
    hbuf,
    g_sem,
    w_sem,
    t_sem,
    tsend,
    trecv,
    rsend,
    rrecv,
    csend,
    crecv,
    s1send,
    s1recv,
    s2send,
    s2recv,
    dsend,
    drecv,
    psend,
    precv,
    hsend,
    hrecv,
):
    f32 = jnp.float32
    my_row = lax.axis_index("row")
    me = lax.axis_index("col")
    row_block, col_block = g.shape[1], g.shape[2]
    hidden_units, features = row_block * rows, col_block * cols
    tiles = row_block // LANES
    lane_tiles = col_block // LANES
    local_tokens = tok_in.shape[0]
    token_block = local_tokens * rows // cols
    width = row_block // chunks
    half = cols // 2
    items = chunks * half

    barrier = pltpu.get_barrier_semaphore()
    for step in range(1, cols):
        pl.semaphore_signal(
            barrier, inc=1, device_id={"col": lax.rem(me + step, cols)}, device_id_type=MESH
        )
    for step in range(1, rows):
        pl.semaphore_signal(
            barrier, inc=1, device_id={"row": lax.rem(my_row + step, rows)}, device_id_type=MESH
        )

    def g_copy(m, t):
        span = pl.ds(t * LANES, LANES)
        return pltpu.make_async_copy(g_in.at[m, span, :], g.at[m, span, :], g_sem.at[m, t])

    def w_copy(m, c):
        span = pl.ds(c * width, width)
        return pltpu.make_async_copy(w_in.at[m, span, :], w.at[m, span, :], w_sem.at[m, c])

    own_tokens = pltpu.make_async_copy(
        tok_in, tok.at[pl.ds(my_row * local_tokens, local_tokens), :], t_sem
    )
    own_tokens.start()
    for m in range(2):
        @pl.loop(0, tiles)
        def _(t):
            g_copy(m, t).start()

    bits = [1 << i for i in reversed(range(rows.bit_length() - 1))]
    orders = [list(bits), list(bits)]
    if len(bits) > 1:
        orders[1][0], orders[1][1] = bits[1], bits[0]
    part_tokens = local_tokens // 2
    counters = [0, 0]
    token_sends = []

    def token_part(h, block):
        return tok.at[pl.ds(block * local_tokens + h * part_tokens, part_tokens), :]

    def token_copy(h, block, peer, slot):
        return pltpu.make_async_remote_copy(
            src_ref=token_part(h, block),
            dst_ref=token_part(h, block),
            send_sem=tsend.at[h, slot],
            recv_sem=trecv.at[h, block],
            device_id={"row": peer},
            device_id_type=MESH,
        )

    def token_send(h, block, mask):
        copy = token_copy(h, block, flip(my_row, mask), counters[h])
        counters[h] += 1
        copy.start()
        token_sends.append(copy)

    def token_wait(h, block):
        token_copy(h, block, flip(my_row, 1), 0).wait_recv()

    def stats(m):
        colacc[m] = jnp.zeros((8, col_block), f32)

        @pl.loop(0, tiles)
        def _(t):
            g_copy(m, t).wait()
            span = pl.ds(pl.multiple_of(t * LANES, LANES), LANES)
            acc = jnp.zeros((LANES, LANES), f32)
            for k in range(lane_tiles):
                lanes = slice(k * LANES, (k + 1) * LANES)
                value = g[m, span, lanes].astype(f32)
                square = value * value
                acc = acc + square
                colacc[m, :, lanes] = colacc[m, :, lanes] + jnp.sum(
                    square.reshape(LANES // 8, 8, LANES), axis=0
                )
            rslot[me, pl.ds(m, 1), span] = jnp.sum(acc.T, axis=0, keepdims=True)

        cslot[my_row, pl.ds(m, 1), :] = jnp.sum(colacc[m], axis=0, keepdims=True)

    def share(ref, axis, count, index, send_sems, recv_sems):
        sends = []
        for step in range(1, count):
            peer = lax.rem(index + step, count)
            copy = pltpu.make_async_remote_copy(
                src_ref=ref.at[index],
                dst_ref=ref.at[index],
                send_sem=send_sems.at[step],
                recv_sem=recv_sems.at[index],
                device_id={axis: peer},
                device_id_type=MESH,
            )
            copy.start()
            sends.append(copy)
        return sends

    def gather(ref, axis, count, index, send_sems, recv_sems):
        for step in range(1, count):
            peer = lax.rem(index + step, count)
            pltpu.make_async_remote_copy(
                src_ref=ref.at[index],
                dst_ref=ref.at[peer],
                send_sem=send_sems.at[step],
                recv_sem=recv_sems.at[peer],
                device_id={axis: peer},
                device_id_type=MESH,
            ).wait_recv()
        total = ref[0]
        for i in range(1, count):
            total = total + ref[i]
        return total

    stats(0)
    pl.semaphore_wait(barrier, cols - 1 + rows - 1)
    own_tokens.wait()
    for h in range(2):
        token_send(h, my_row, orders[h][0])
    stats(1)
    sends = share(rslot, "col", cols, me, rsend, rrecv)
    sends += share(cslot, "row", rows, my_row, csend, crecv)
    for h in range(2):
        for mask in orders[h][1:]:
            token_send(h, my_row, mask)
    for h in range(2):
        block = flip(my_row, orders[h][0])
        token_wait(h, block)
        for mask in orders[h][1:]:
            token_send(h, block, mask)

    @pl.loop(0, chunks)
    def _(c):
        w_copy(0, c).start()
        w_copy(1, c).start()

    row_total = gather(rslot, "col", cols, me, rsend, rrecv)
    row_new = decay_rate * rf_ref[...] + (1.0 - decay_rate) * (row_total / features + tiny_eps)
    row_out[...] = row_new
    row_root = jnp.sqrt(1.0 / row_new)
    for m in range(2):
        for t in range(tiles):
            lanes = slice(t * LANES, (t + 1) * LANES)
            rcol[m, lanes, :] = jnp.broadcast_to(row_root[m : m + 1, lanes], (LANES, LANES)).T
    col_total = gather(cslot, "row", rows, my_row, csend, crecv)
    col_new = decay_rate * cf_ref[...] + (1.0 - decay_rate) * (col_total / hidden_units + tiny_eps)
    col_out[...] = col_new
    cgain[...] = 1.0 / col_new

    s1[me] = jnp.zeros((8, LANES), f32)
    for m in range(2):
        def tile_norm(t, total):
            span = pl.ds(pl.multiple_of(t * LANES, LANES), LANES)
            acc = jnp.zeros((LANES, LANES), f32)
            for k in range(lane_tiles):
                lanes = slice(k * LANES, (k + 1) * LANES)
                value = g[m, span, lanes].astype(f32)
                acc = acc + value * value * cgain[pl.ds(m, 1), lanes]
            root = rcol[m, span, :]
            acc = acc * root * root
            return total + jnp.sum(acc.reshape(LANES // 8, 8, LANES), axis=0)

        total = lax.fori_loop(0, tiles, tile_norm, jnp.zeros((8, LANES), f32))
        s1[me, pl.ds(m, 1), :] = jnp.sum(total, axis=0, keepdims=True)

    sends += share(s1, "col", cols, me, s1send, s1recv)
    row_sum = row_new[:, :LANES]
    for t in range(1, tiles):
        row_sum = row_sum + row_new[:, t * LANES : (t + 1) * LANES]
    s2[my_row] = jnp.zeros((8, LANES), f32)
    s2[my_row, 2:4, :] = row_sum
    norm = gather(s1, "col", cols, me, s1send, s1recv)
    s2[my_row, 0:2, :] = norm[0:2, :]
    sends += share(s2, "row", rows, my_row, s2send, s2recv)

    for step in range(1, len(bits) - 1):
        for h in range(2):
            peer = flip(my_row, orders[h][step])
            for block in subsets(peer, orders[h][:step]):
                token_wait(h, block)
                for mask in orders[h][step + 1 :]:
                    token_send(h, block, mask)

    totals = gather(s2, "row", rows, my_row, s2send, s2recv)
    totals = jnp.sum(totals, axis=1, keepdims=True)
    for m in range(2):
        row_mean = totals[m + 2 : m + 3, :] / hidden_units
        mean_square = row_mean * totals[m : m + 1, :] / (hidden_units * features)
        clip_scale = jnp.maximum(1.0, jnp.sqrt(mean_square) / clip_limit)
        rate = jnp.sqrt(row_mean) * (learn_rate / clip_scale)
        cgain[pl.ds(m, 1), :] = jnp.sqrt(cgain[pl.ds(m, 1), :]) * rate

    for h in range(2):
        peer = flip(my_row, orders[h][-1])
        for block in subsets(peer, orders[h][:-1]):
            token_wait(h, block)

    def renew(c):
        for m in range(2):
            w_copy(m, c).wait()

            @pl.loop(0, width // STRIP)
            def _(i):
                span = pl.ds(pl.multiple_of(c * width + i * STRIP, STRIP), STRIP)
                root = rcol[m, span, :]
                for k in range(lane_tiles):
                    lanes = slice(k * LANES, (k + 1) * LANES)
                    step = g[m, span, lanes].astype(f32) * root * cgain[pl.ds(m, 1), lanes]
                    w[m, span, lanes] = (w[m, span, lanes].astype(f32) - step).astype(jnp.bfloat16)

    def product(b, c):
        chosen = tok[pl.ds(pl.multiple_of(b * token_block, token_block), token_block), :]
        span = pl.ds(pl.multiple_of(c * width, width), width)
        for m in range(2):
            prod[:, m * width : (m + 1) * width] = lax.dot_general(
                chosen, w[m, span, :], (((1,), (1,)), ((), ())), preferred_element_type=f32
            )

    def data_copy(d, k):
        return pltpu.make_async_remote_copy(
            src_ref=sbuf.at[d, k],
            dst_ref=rbuf.at[d, k],
            send_sem=dsend.at[d, k],
            recv_sem=drecv.at[d, k],
            device_id={"col": me + 2 * d - 1},
            device_id_type=MESH,
        )

    def peak_copy(d, k):
        return pltpu.make_async_remote_copy(
            src_ref=sscale.at[d, k],
            dst_ref=rscale.at[d, k],
            send_sem=psend.at[d, k],
            recv_sem=precv.at[d, k],
            device_id={"col": me + 2 * d - 1},
            device_id_type=MESH,
        )

    def add_received(d, k):
        peak_copy(d, k).wait_recv()
        data_copy(d, k).wait_recv()
        unit = rscale[d, k] / code_span

        @pl.loop(0, token_block // STRIP)
        def _(i):
            span = pl.ds(pl.multiple_of(i * STRIP, STRIP), STRIP)
            code = rbuf[d, k, span, :].astype(f32)
            value = (jnp.log2(jnp.abs(code)) + 0.5 * code_span) * unit
            prod[span, :] = prod[span, :] + jnp.where(code < 0, -value, value)

    def send_on(d, k):
        def strip_peak(i, peak):
            span = pl.ds(pl.multiple_of(i * STRIP, STRIP), STRIP)
            part = jnp.abs(prod[span, :])
            return jnp.maximum(peak, jnp.max(part.reshape(STRIP // 8, 8, 2 * width), axis=0))

        peak = lax.fori_loop(0, token_block // STRIP, strip_peak, jnp.zeros((8, 2 * width), f32))
        peak = jnp.maximum(jnp.max(peak, axis=0, keepdims=True), 1e-30)
        sscale[d, k] = peak
        peak_copy(d, k).start()
        unit = code_span / peak

        @pl.loop(0, token_block // STRIP)
        def _(i):
            span = pl.ds(pl.multiple_of(i * STRIP, STRIP), STRIP)
            part = prod[span, :]
            size = jnp.exp2(jnp.abs(part) * unit - 0.5 * code_span)
            sbuf[d, k, span, :] = jnp.where(part < 0, -size, size).astype(jnp.bfloat16)

        data_copy(d, k).start()

    def block_of(d, k):
        turn = lax.rem(k, half)
        return d * (half + turn) + (1 - d) * (half - 1 - turn)

    def hidden_copy(k):
        c = k // half
        return pltpu.make_async_remote_copy(
            src_ref=hbuf.at[k],
            dst_ref=out_ref.at[:, pl.ds(pl.multiple_of(c * width, width), width)],
            send_sem=hsend.at[k],
            recv_sem=hrecv.at[c],
            device_id={"col": block_of(far, k)},
            device_id_type=MESH,
        )

    def finish(k):
        b = block_of(far, k)
        columns = pl.ds(pl.multiple_of((k // half) * width, width), width)

        @pl.loop(0, token_block // STRIP)
        def _(i):
            span = pl.ds(pl.multiple_of(i * STRIP, STRIP), STRIP)
            gate = prod[span, 0:width]
            value = (gate / (1.0 + jnp.exp(-gate)) * prod[span, width:]).astype(jnp.bfloat16)
            hbuf[k, span, :] = value

        @pl.when(b == me)
        def _():
            out_ref[:, columns] = hbuf[k]

        @pl.when(b != me)
        def _():
            hidden_copy(k).start()

    near = 1 - me // half
    far = 1 - near
    depth = near * me + far * (cols - 1 - me)
    inner = (depth + half - 1) // half
    lag = END_LAG + inner * (INNER_LAG - END_LAG)

    @pl.loop(0, items + max(END_LAG, INNER_LAG))
    def _(k):
        @pl.when(k < items)
        def _():
            c = k // half

            @pl.when(lax.rem(k, half) == 0)
            def _():
                renew(c)

            product(block_of(near, k), c)

            @pl.when(depth > 0)
            def _():
                add_received(near, k)

            send_on(near, k)

        @pl.when((k >= lag) & (k < items + lag))
        def _():
            j = k - lag
            product(block_of(far, j), j // half)
            add_received(far, j)

            @pl.when(depth > 0)
            def _():
                send_on(far, j)

            @pl.when(depth == 0)
            def _():
                finish(j)

    for copy in sends:
        copy.wait_send()
    for copy in token_sends:
        copy.wait_send()

    @pl.loop(0, items)
    def _(k):
        data_copy(near, k).wait_send()
        peak_copy(near, k).wait_send()

        @pl.when(depth > 0)
        def _():
            data_copy(far, k).wait_send()
            peak_copy(far, k).wait_send()

        @pl.when((depth == 0) & (block_of(far, k) != me))
        def _():
            hidden_copy(k).wait_send()

    @pl.when(depth > 0)
    def _():
        @pl.loop(0, chunks)
        def _(c):
            hidden_copy(c * half).wait_recv()


def local(rows, cols, tokens, weights, gradients, row_factors, col_factors):
    row_block, col_block = gradients.shape[1], gradients.shape[2]
    all_tokens = tokens.shape[0] * rows
    token_block = all_tokens // cols
    chunks = max(n for n in (1, 2, 3, 4, 5, 6, 7) if row_block % (n * LANES) == 0)
    width = row_block // chunks
    items = chunks * (cols // 2)
    tiles = row_block // LANES
    f32, bf16 = jnp.float32, jnp.bfloat16
    vmem = pl.BlockSpec(memory_space=pltpu.VMEM)
    anywhere = pl.BlockSpec(memory_space=pl.ANY)
    dma = pltpu.SemaphoreType.DMA
    return pl.pallas_call(
        functools.partial(body, rows, cols, chunks),
        out_shape=(
            jax.ShapeDtypeStruct((token_block, row_block), bf16),
            jax.ShapeDtypeStruct((2, row_block), f32),
            jax.ShapeDtypeStruct((2, col_block), f32),
        ),
        in_specs=[anywhere, anywhere, anywhere, vmem, vmem],
        out_specs=(vmem, vmem, vmem),
        scratch_shapes=[
            pltpu.VMEM((all_tokens, col_block), bf16),
            pltpu.VMEM((2, row_block, col_block), bf16),
            pltpu.VMEM((2, row_block, col_block), bf16),
            pltpu.VMEM((2, row_block, LANES), f32),
            pltpu.VMEM((2, 8, col_block), f32),
            pltpu.VMEM((2, col_block), f32),
            pltpu.VMEM((cols, 2, row_block), f32),
            pltpu.VMEM((rows, 2, col_block), f32),
            pltpu.VMEM((cols, 8, LANES), f32),
            pltpu.VMEM((rows, 8, LANES), f32),
            pltpu.VMEM((token_block, 2 * width), f32),
            pltpu.VMEM((2, items, token_block, 2 * width), bf16),
            pltpu.VMEM((2, items, token_block, 2 * width), bf16),
            pltpu.VMEM((2, items, 1, 2 * width), f32),
            pltpu.VMEM((2, items, 1, 2 * width), f32),
            pltpu.VMEM((items, token_block, width), bf16),
            dma((2, tiles)),
            dma((2, chunks)),
            dma,
            dma((2, rows)),
            dma((2, rows)),
            dma((cols,)),
            dma((cols,)),
            dma((rows,)),
            dma((rows,)),
            dma((cols,)),
            dma((cols,)),
            dma((rows,)),
            dma((rows,)),
            dma((2, items)),
            dma((2, items)),
            dma((2, items)),
            dma((2, items)),
            dma((items,)),
            dma((chunks,)),
        ],
        compiler_params=pltpu.CompilerParams(
            collective_id=0, has_side_effects=True, vmem_limit_bytes=67000000
        ),
    )(tokens, weights, gradients, row_factors, col_factors)


def solution(mesh):
    placed = (
        P("row", "col"),
        P(None, "row", "col"),
        P(None, "row", "col"),
        P(None, "row"),
        P(None, "col"),
    )
    return jax.shard_map(
        functools.partial(local, mesh.shape["row"], mesh.shape["col"]),
        mesh=mesh,
        in_specs=placed,
        out_specs=(P("col", "row"), P(None, "row"), P(None, "col")),
        check_vma=False,
    )
```

```python
import functools
import jax
import jax.numpy as jnp
from jax import lax
from jax.experimental import pallas as pl
from jax.experimental.pallas import tpu as pltpu
from jax.sharding import PartitionSpec as P

decay_rate = 0.5
learn_rate = 0.01
clip_limit = 1.0
tiny_eps = 1e-30
code_span = 250.0


MESH = pl.DeviceIdType.MESH
LANES = 128
STRIP = 32
INNER_LAG = 1
PARTS = 4


def flip(value, mask):
    return value + mask * (1 - 2 * ((value // mask) % 2))


def flips(value, masks):
    for mask in masks:
        value = flip(value, mask)
    return value


def subsets(masks):
    out = [()]
    for mask in masks:
        out = out + [item + (mask,) for item in out]
    return out


def body(
    rows,
    cols,
    chunks,
    tok_in,
    w_in,
    g_in,
    rf_ref,
    cf_ref,
    out_ref,
    row_out,
    col_out,
    tok,
    w,
    g,
    rcol,
    colacc,
    cgain,
    rnew,
    cnew,
    rnorm,
    rslot,
    cslot,
    s1,
    s2,
    prod,
    sbuf,
    rbuf,
    sscale,
    rscale,
    hbuf,
    o_sem,
    lsend,
    g_sem,
    w_sem,
    t_sem,
    tsend,
    trecv,
    rsend,
    rrecv,
    csend,
    crecv,
    s1send,
    s1recv,
    s2send,
    s2recv,
    dsend,
    drecv,
    psend,
    precv,
    hsend,
    hrecv,
):
    f32 = jnp.float32
    my_row = lax.axis_index("row")
    me = lax.axis_index("col")
    row_block, col_block = g.shape[1], g.shape[2]
    hidden_units, features = row_block * rows, col_block * cols
    tiles = row_block // LANES
    lane_tiles = col_block // LANES
    local_tokens = tok_in.shape[0]
    token_block = local_tokens * rows // cols
    width = row_block // chunks
    half = cols // 2
    items = chunks * half

    barrier = pltpu.get_barrier_semaphore()
    for step in range(1, cols):
        pl.semaphore_signal(
            barrier, inc=1, device_id={"col": lax.rem(me + step, cols)}, device_id_type=MESH
        )
    for step in range(1, rows):
        pl.semaphore_signal(
            barrier, inc=1, device_id={"row": lax.rem(my_row + step, rows)}, device_id_type=MESH
        )

    def g_copy(m, t):
        span = pl.ds(t * LANES, LANES)
        return pltpu.make_async_copy(g_in.at[m, span, :], g.at[m, span, :], g_sem.at[m, t])

    def w_copy(m, c):
        span = pl.ds(c * width, width)
        return pltpu.make_async_copy(
            w_in.at[m, span, :], w.at[c, pl.ds(m * width, width), :], w_sem.at[m, c]
        )

    own_tokens = pltpu.make_async_copy(
        tok_in, tok.at[pl.ds(my_row * local_tokens, local_tokens), :], t_sem
    )
    for m in range(2):
        @pl.loop(0, tiles)
        def _(t):
            g_copy(m, t).start()

    own_tokens.start()

    bits = [1 << i for i in reversed(range(rows.bit_length() - 1))]
    swapped = [bits[1], bits[0]] + bits[2:] if len(bits) > 2 else bits
    orders = [swapped if h % 2 else bits for h in range(PARTS)]
    part_tokens = local_tokens // PARTS
    counters = [0] * PARTS
    token_sends = []

    def token_copy(h, masks, mask, slot):
        block = flips(my_row, masks)
        part = tok.at[pl.ds(block * local_tokens + h * part_tokens, part_tokens), :]
        return pltpu.make_async_remote_copy(
            src_ref=part,
            dst_ref=part,
            send_sem=tsend.at[h, slot],
            recv_sem=trecv.at[h, block],
            device_id={"row": flip(my_row, mask)},
            device_id_type=MESH,
        )

    def token_send(h, masks, mask):
        token_copy(h, masks, mask, counters[h]).start()
        token_sends.append((h, masks, mask, counters[h]))
        counters[h] += 1

    def token_wait(h, masks):
        token_copy(h, masks, masks[-1], 0).wait_recv()

    def stats(m):
        colacc[m] = jnp.zeros((8, col_block), f32)

        @pl.loop(0, tiles)
        def _(t):
            g_copy(m, t).wait()
            span = pl.ds(pl.multiple_of(t * LANES, LANES), LANES)
            acc = jnp.zeros((LANES, LANES), f32)
            for k in range(lane_tiles):
                lanes = slice(k * LANES, (k + 1) * LANES)
                value = g[m, span, lanes].astype(f32)
                square = value * value
                acc = acc + square
                colacc[m, :, lanes] = colacc[m, :, lanes] + jnp.sum(
                    square.reshape(LANES // 8, 8, LANES), axis=0
                )
            rslot[m, me, :, span] = jnp.sum(acc.T, axis=0, keepdims=True)

        cslot[m, my_row] = jnp.sum(colacc[m], axis=0, keepdims=True)

    def share(ref, axis, count, index, send_sems, recv_sems):
        sends = []
        for step in range(1, count):
            peer = lax.rem(index + step, count)
            copy = pltpu.make_async_remote_copy(
                src_ref=ref.at[index],
                dst_ref=ref.at[index],
                send_sem=send_sems.at[step],
                recv_sem=recv_sems.at[index],
                device_id={axis: peer},
                device_id_type=MESH,
            )
            copy.start()
            sends.append(copy)
        return sends

    def gather(ref, axis, count, index, send_sems, recv_sems):
        for step in range(1, count):
            peer = lax.rem(index + step, count)
            pltpu.make_async_remote_copy(
                src_ref=ref.at[index],
                dst_ref=ref.at[peer],
                send_sem=send_sems.at[step],
                recv_sem=recv_sems.at[peer],
                device_id={axis: peer},
                device_id_type=MESH,
            ).wait_recv()
        total = ref[0]
        for i in range(1, count):
            total = total + ref[i]
        return total

    def share_factors(m):
        out = share(cslot.at[m], "row", rows, my_row, csend.at[m], crecv.at[m])
        return out + share(rslot.at[m], "col", cols, me, rsend.at[m], rrecv.at[m])

    stats(0)
    pl.semaphore_wait(barrier, cols - 1 + rows - 1)
    sends = share_factors(0)
    own_tokens.wait()
    for h in range(PARTS // 2):
        token_send(h, (), orders[h][0])
    for h in range(PARTS // 2):
        token_send(h, (), orders[h][-1])
    stats(1)
    sends += share_factors(1)
    for h in range(PARTS // 2, PARTS):
        token_send(h, (), orders[h][0])
    for h in range(PARTS):
        for mask in orders[h][1:-1]:
            token_send(h, (), mask)
    for h in range(PARTS // 2, PARTS):
        token_send(h, (), orders[h][-1])

    @pl.loop(0, chunks)
    def _(c):
        w_copy(0, c).start()
        w_copy(1, c).start()

    for m in range(2):
        col_total = gather(cslot.at[m], "row", rows, my_row, csend.at[m], crecv.at[m])
        col_new = decay_rate * cf_ref[pl.ds(m, 1), :] + (1.0 - decay_rate) * (
            col_total / hidden_units + tiny_eps
        )
        cnew[pl.ds(m, 1), :] = col_new
        cgain[pl.ds(m, 1), :] = 1.0 / col_new

        @pl.loop(0, tiles)
        def _(t):
            span = pl.ds(pl.multiple_of(t * LANES, LANES), LANES)
            acc = jnp.zeros((LANES, LANES), f32)
            for k in range(lane_tiles):
                lanes = slice(k * LANES, (k + 1) * LANES)
                value = g[m, span, lanes].astype(f32)
                acc = acc + value * value * cgain[pl.ds(m, 1), lanes]
            rnorm[pl.ds(m, 1), span] = jnp.sum(acc.T, axis=0, keepdims=True)

    def lane_sum(value):
        total = value[:, :LANES]
        for t in range(1, tiles):
            total = total + value[:, t * LANES : (t + 1) * LANES]
        return total

    s1[me] = jnp.zeros((8, LANES), f32)
    s2[my_row] = jnp.zeros((8, LANES), f32)
    for m in range(2):
        row_total = gather(rslot.at[m], "col", cols, me, rsend.at[m], rrecv.at[m])
        row_new = decay_rate * rf_ref[pl.ds(m, 1), :] + (1.0 - decay_rate) * (
            row_total / features + tiny_eps
        )
        rnew[pl.ds(m, 1), :] = row_new
        s1[me, pl.ds(m, 1), :] = lane_sum(rnorm[pl.ds(m, 1), :] / row_new)

    sends += share(s1, "col", cols, me, s1send, s1recv)
    row_copy = pltpu.make_async_copy(rnew, row_out, o_sem.at[0])
    row_copy.start()
    col_copy = pltpu.make_async_copy(cnew, col_out, o_sem.at[1])
    col_copy.start()
    s2[my_row, 2:4, :] = lane_sum(rnew[...])
    row_root = jnp.sqrt(1.0 / rnew[...])
    for m in range(2):
        for t in range(tiles):
            lanes = slice(t * LANES, (t + 1) * LANES)
            rcol[m, lanes, :] = jnp.broadcast_to(row_root[m : m + 1, lanes], (LANES, LANES)).T
    norm = gather(s1, "col", cols, me, s1send, s1recv)
    s2[my_row, 0:2, :] = norm[0:2, :]
    sends += share(s2, "row", rows, my_row, s2send, s2recv)

    defer = len(bits) == 3 and half == 2
    for h in range(PARTS):
        token_wait(h, (orders[h][0],))
        for mask in orders[h][1:]:
            token_send(h, (orders[h][0],), mask)
    for h in range(PARTS):
        token_wait(h, (orders[h][1],))
        for mask in orders[h][2:]:
            token_send(h, (orders[h][1],), mask)

    totals = gather(s2, "row", rows, my_row, s2send, s2recv)
    totals = jnp.sum(totals, axis=1, keepdims=True)
    for m in range(2):
        row_mean = totals[m + 2 : m + 3, :] / hidden_units
        mean_square = row_mean * totals[m : m + 1, :] / (hidden_units * features)
        clip_scale = jnp.maximum(1.0, jnp.sqrt(mean_square) / clip_limit)
        rate = jnp.sqrt(row_mean) * (learn_rate / clip_scale)
        cgain[pl.ds(m, 1), :] = jnp.sqrt(cgain[pl.ds(m, 1), :]) * rate

    early = [(), (0,), (1,)]
    for h in range(PARTS):
        for picks in early:
            token_wait(h, tuple(orders[h][i] for i in picks) + (orders[h][-1],))

    def late_tokens():
        for step in range(1, len(bits) - 1):
            for h in range(PARTS):
                for before in subsets(orders[h][:step]):
                    if step == 1 and not before:
                        continue
                    masks = before + (orders[h][step],)
                    token_wait(h, masks)
                    for mask in orders[h][step + 1 :]:
                        token_send(h, masks, mask)
        for h in range(PARTS):
            for before in subsets(orders[h][:-1]):
                if before in [tuple(orders[h][i] for i in picks) for picks in early]:
                    continue
                token_wait(h, before + (orders[h][-1],))

    if not defer:
        late_tokens()

    def renew(c):
        for m in range(2):
            w_copy(m, c).wait()

            @pl.loop(0, width // STRIP)
            def _(i):
                span = pl.ds(pl.multiple_of(c * width + i * STRIP, STRIP), STRIP)
                here = pl.ds(pl.multiple_of(m * width + i * STRIP, STRIP), STRIP)
                root = rcol[m, span, :]
                for k in range(lane_tiles):
                    lanes = slice(k * LANES, (k + 1) * LANES)
                    step = g[m, span, lanes].astype(f32) * root * cgain[pl.ds(m, 1), lanes]
                    w[c, here, lanes] = (w[c, here, lanes].astype(f32) - step).astype(jnp.bfloat16)

    def product(b, c):
        chosen = tok[pl.ds(pl.multiple_of(b * token_block, token_block), token_block), :]
        prod[...] = lax.dot_general(
            chosen, w[c], (((1,), (1,)), ((), ())), preferred_element_type=f32
        )

    def data_copy(d, k):
        return pltpu.make_async_remote_copy(
            src_ref=sbuf.at[d, k],
            dst_ref=rbuf.at[d, k],
            send_sem=dsend.at[d, k],
            recv_sem=drecv.at[d, k],
            device_id={"col": me + 2 * d - 1},
            device_id_type=MESH,
        )

    def peak_copy(d, k):
        return pltpu.make_async_remote_copy(
            src_ref=sscale.at[d, k],
            dst_ref=rscale.at[d, k],
            send_sem=psend.at[d, k],
            recv_sem=precv.at[d, k],
            device_id={"col": me + 2 * d - 1},
            device_id_type=MESH,
        )

    def add_received(d, k):
        peak_copy(d, k).wait_recv()
        data_copy(d, k).wait_recv()
        unit = rscale[d, k] / code_span

        @pl.loop(0, token_block // STRIP)
        def _(i):
            span = pl.ds(pl.multiple_of(i * STRIP, STRIP), STRIP)
            code = rbuf[d, k, span, :].astype(f32)
            value = (jnp.log2(jnp.abs(code)) + 0.5 * code_span) * unit
            prod[span, :] = prod[span, :] + jnp.where(code < 0, -value, value)

    def send_on(d, k):
        def strip_peak(i, peak):
            span = pl.ds(pl.multiple_of(i * STRIP, STRIP), STRIP)
            part = jnp.abs(prod[span, :])
            return jnp.maximum(peak, jnp.max(part.reshape(STRIP // 8, 8, 2 * width), axis=0))

        peak = lax.fori_loop(0, token_block // STRIP, strip_peak, jnp.zeros((8, 2 * width), f32))
        peak = jnp.maximum(jnp.max(peak, axis=0, keepdims=True), 1e-30)
        sscale[d, k] = peak
        peak_copy(d, k).start()
        unit = code_span / peak

        @pl.loop(0, token_block // STRIP)
        def _(i):
            span = pl.ds(pl.multiple_of(i * STRIP, STRIP), STRIP)
            part = prod[span, :]
            size = jnp.exp2(jnp.abs(part) * unit - 0.5 * code_span)
            sbuf[d, k, span, :] = jnp.where(part < 0, -size, size).astype(jnp.bfloat16)

        data_copy(d, k).start()

    def block_of(d, k):
        return d * half + lax.rem(k + my_row // 2, half)

    def hidden_copy(k):
        c = k // half
        return pltpu.make_async_remote_copy(
            src_ref=hbuf.at[k],
            dst_ref=out_ref.at[:, pl.ds(pl.multiple_of(c * width, width), width)],
            send_sem=hsend.at[k],
            recv_sem=hrecv.at[c],
            device_id={"col": block_of(far, k)},
            device_id_type=MESH,
        )

    def local_copy(k):
        c = k // half
        return pltpu.make_async_copy(
            hbuf.at[k],
            out_ref.at[:, pl.ds(pl.multiple_of(c * width, width), width)],
            lsend.at[k],
        )

    def finish(k):
        b = block_of(far, k)

        @pl.loop(0, token_block // STRIP)
        def _(i):
            span = pl.ds(pl.multiple_of(i * STRIP, STRIP), STRIP)
            gate = prod[span, 0:width]
            value = (gate / (1.0 + jnp.exp(-gate)) * prod[span, width:]).astype(jnp.bfloat16)
            hbuf[k, span, :] = value

        @pl.when(b == me)
        def _():
            local_copy(k).start()

        @pl.when(b != me)
        def _():
            hidden_copy(k).start()

    near = 1 - me // half
    far = 1 - near
    depth = near * me + far * (cols - 1 - me)
    inner = (depth + half - 1) // half
    lag = items + inner * (INNER_LAG - items)

    @pl.loop(0, 2 * items)
    def _(k):
        @pl.when(k < items)
        def _():
            c = k // half

            if defer:
                pl.when(k == 1)(late_tokens)

            @pl.when(lax.rem(k, half) == 0)
            def _():
                renew(c)

            product(block_of(near, k), c)

            @pl.when(depth > 0)
            def _():
                add_received(near, k)

            send_on(near, k)

        @pl.when((k >= lag) & (k < items + lag))
        def _():
            j = k - lag
            product(block_of(far, j), j // half)
            add_received(far, j)

            @pl.when(depth > 0)
            def _():
                send_on(far, j)

            @pl.when(depth == 0)
            def _():
                finish(j)

    for copy in sends:
        copy.wait_send()
    for item in token_sends:
        token_copy(*item).wait_send()
    row_copy.wait()
    col_copy.wait()

    @pl.loop(0, items)
    def _(k):
        data_copy(near, k).wait_send()
        peak_copy(near, k).wait_send()

        @pl.when(depth > 0)
        def _():
            data_copy(far, k).wait_send()
            peak_copy(far, k).wait_send()

        @pl.when((depth == 0) & (block_of(far, k) != me))
        def _():
            hidden_copy(k).wait_send()

        @pl.when((depth == 0) & (block_of(far, k) == me))
        def _():
            local_copy(k).wait()

    @pl.when(depth > 0)
    def _():
        @pl.loop(0, chunks)
        def _(c):
            hidden_copy(c * half).wait_recv()


def settle(h_in, r_in, c_in, h_out, r_out, c_out, h_buf, r_buf, c_buf, sems):
    pieces = 4
    depth = h_in.shape[0] // pieces
    moves = [(r_in, r_buf, r_out), (c_in, c_buf, c_out)]
    for i in range(pieces):
        span = pl.ds(i * depth, depth)
        moves.append((h_in.at[span, :], h_buf.at[span, :], h_out.at[span, :]))
    loads = [
        pltpu.make_async_copy(a, b, sems.at[0, i]) for i, (a, b, _) in enumerate(moves)
    ]
    stores = [
        pltpu.make_async_copy(b, c, sems.at[1, i]) for i, (_, b, c) in enumerate(moves)
    ]
    for load in loads:
        load.start()
    for load, store in zip(loads, stores):
        load.wait()
        store.start()
    for store in stores:
        store.wait()


def local(rows, cols, tokens, weights, gradients, row_factors, col_factors):
    row_block, col_block = gradients.shape[1], gradients.shape[2]
    all_tokens = tokens.shape[0] * rows
    token_block = all_tokens // cols
    chunks = max(n for n in (1, 2, 3, 4, 5, 6, 7) if row_block % (n * LANES) == 0)
    width = row_block // chunks
    items = chunks * (cols // 2)
    tiles = row_block // LANES
    f32, bf16 = jnp.float32, jnp.bfloat16
    vmem = pl.BlockSpec(memory_space=pltpu.VMEM)
    anywhere = pl.BlockSpec(memory_space=pl.ANY)
    dma = pltpu.SemaphoreType.DMA
    shapes = (
        jax.ShapeDtypeStruct((token_block, row_block), bf16),
        jax.ShapeDtypeStruct((2, row_block), f32),
        jax.ShapeDtypeStruct((2, col_block), f32),
    )
    results = pl.pallas_call(
        functools.partial(body, rows, cols, chunks),
        out_shape=shapes,
        in_specs=[anywhere, anywhere, anywhere, vmem, vmem],
        out_specs=(anywhere, anywhere, anywhere),
        scratch_shapes=[
            pltpu.VMEM((all_tokens, col_block), bf16),
            pltpu.VMEM((chunks, 2 * width, col_block), bf16),
            pltpu.VMEM((2, row_block, col_block), bf16),
            pltpu.VMEM((2, row_block, LANES), f32),
            pltpu.VMEM((2, 8, col_block), f32),
            pltpu.VMEM((2, col_block), f32),
            pltpu.VMEM((2, row_block), f32),
            pltpu.VMEM((2, col_block), f32),
            pltpu.VMEM((2, row_block), f32),
            pltpu.VMEM((2, cols, 1, row_block), f32),
            pltpu.VMEM((2, rows, 1, col_block), f32),
            pltpu.VMEM((cols, 8, LANES), f32),
            pltpu.VMEM((rows, 8, LANES), f32),
            pltpu.VMEM((token_block, 2 * width), f32),
            pltpu.VMEM((2, items, token_block, 2 * width), bf16),
            pltpu.VMEM((2, items, token_block, 2 * width), bf16),
            pltpu.VMEM((2, items, 1, 2 * width), f32),
            pltpu.VMEM((2, items, 1, 2 * width), f32),
            pltpu.VMEM((items, token_block, width), bf16),
            dma((2,)),
            dma((items,)),
            dma((2, tiles)),
            dma((2, chunks)),
            dma,
            dma((PARTS, rows)),
            dma((PARTS, rows)),
            dma((2, cols)),
            dma((2, cols)),
            dma((2, rows)),
            dma((2, rows)),
            dma((cols,)),
            dma((cols,)),
            dma((rows,)),
            dma((rows,)),
            dma((2, items)),
            dma((2, items)),
            dma((2, items)),
            dma((2, items)),
            dma((items,)),
            dma((chunks,)),
        ],
        compiler_params=pltpu.CompilerParams(
            collective_id=0, has_side_effects=True, vmem_limit_bytes=67000000
        ),
    )(tokens, weights, gradients, row_factors, col_factors)
    return pl.pallas_call(
        settle,
        out_shape=shapes,
        in_specs=[anywhere, anywhere, anywhere],
        out_specs=(anywhere, anywhere, anywhere),
        scratch_shapes=[
            pltpu.VMEM((token_block, row_block), bf16),
            pltpu.VMEM((2, row_block), f32),
            pltpu.VMEM((2, col_block), f32),
            dma((2, 6)),
        ],
    )(*results)


def solution(mesh):
    placed = (
        P("row", "col"),
        P(None, "row", "col"),
        P(None, "row", "col"),
        P(None, "row"),
        P(None, "col"),
    )
    return jax.shard_map(
        functools.partial(local, mesh.shape["row"], mesh.shape["col"]),
        mesh=mesh,
        in_specs=placed,
        out_specs=(P("col", "row"), P(None, "row"), P(None, "col")),
        check_vma=False,
    )
```

```python
import functools
import jax
import jax.numpy as jnp
from jax import lax
from jax.experimental import pallas as pl
from jax.experimental.pallas import tpu as pltpu
from jax.sharding import PartitionSpec as P

decay_rate = 0.5
learn_rate = 0.01
clip_limit = 1.0
tiny_eps = 1e-30
code_span = 250.0


MESH = pl.DeviceIdType.MESH
LANES = 128
STRIP = 32
INNER_LAG = 2
CUTS = ((0, 2), (2, 3), (5, 3))
PARTS = len(CUTS)
FIRST = 1


def flip(value, mask):
    return value + mask * (1 - 2 * ((value // mask) % 2))


def flips(value, masks):
    for mask in masks:
        value = flip(value, mask)
    return value


def subsets(masks):
    out = [()]
    for mask in masks:
        out = out + [item + (mask,) for item in out]
    return out


def body(
    rows,
    cols,
    chunks,
    tok_in,
    w_in,
    g_in,
    rf_ref,
    cf_ref,
    out_ref,
    row_out,
    col_out,
    tok,
    w,
    g,
    rcol,
    colacc,
    cgain,
    rnew,
    cnew,
    rnorm,
    rslot,
    cslot,
    s1,
    s2,
    prod,
    kept,
    sbuf,
    rbuf,
    sscale,
    rscale,
    hbuf,
    o_sem,
    lsend,
    g_sem,
    w_sem,
    t_sem,
    tsend,
    trecv,
    rsend,
    rrecv,
    csend,
    crecv,
    s1send,
    s1recv,
    s2send,
    s2recv,
    dsend,
    drecv,
    psend,
    precv,
    hsend,
    hrecv,
):
    f32 = jnp.float32
    my_row = lax.axis_index("row")
    me = lax.axis_index("col")
    row_block, col_block = g.shape[1], g.shape[2]
    hidden_units, features = row_block * rows, col_block * cols
    tiles = row_block // LANES
    lane_tiles = col_block // LANES
    local_tokens = tok_in.shape[0]
    token_block = local_tokens * rows // cols
    width = row_block // chunks
    half = cols // 2
    items = 2 * chunks * half

    barrier = pltpu.get_barrier_semaphore()
    for step in range(1, cols):
        pl.semaphore_signal(
            barrier, inc=1, device_id={"col": lax.rem(me + step, cols)}, device_id_type=MESH
        )
    for step in range(1, rows):
        pl.semaphore_signal(
            barrier, inc=1, device_id={"row": lax.rem(my_row + step, rows)}, device_id_type=MESH
        )

    group = 2 if tiles % 2 == 0 else 1

    def g_copy(t):
        span = pl.ds(t * LANES * group, LANES * group)
        return pltpu.make_async_copy(g_in.at[0, span, :], g.at[0, span, :], g_sem.at[t])

    later_g = pltpu.make_async_copy(g_in.at[1], g.at[1], g_sem.at[tiles // group])
    all_w = pltpu.make_async_copy(w_in, w, w_sem)

    own_tokens = pltpu.make_async_copy(
        tok_in, tok.at[pl.ds(my_row * local_tokens, local_tokens), :], t_sem
    )
    @pl.loop(0, tiles // group)
    def _(t):
        g_copy(t).start()

    later_g.start()
    own_tokens.start()

    bits = [1 << i for i in reversed(range(rows.bit_length() - 1))]
    eighth = local_tokens // 8

    def token_copy(h, masks, mask):
        block = flips(my_row, masks)
        first, size = CUTS[h]
        part = tok.at[pl.ds(block * local_tokens + first * eighth, size * eighth), :]
        return pltpu.make_async_remote_copy(
            src_ref=part,
            dst_ref=part,
            send_sem=tsend,
            recv_sem=trecv.at[h, block],
            device_id={"row": flip(my_row, mask)},
            device_id_type=MESH,
        )

    def token_send(h, masks, mask):
        token_copy(h, masks, mask).start()

    def token_wait(h, masks):
        token_copy(h, masks, masks[-1]).wait_recv()

    def stats(m):
        colacc[m] = jnp.zeros((8, col_block), f32)

        if m == 1:
            later_g.wait()

        @pl.loop(0, tiles)
        def _(t):
            if m == 0:
                @pl.when(lax.rem(t, group) == 0)
                def _():
                    g_copy(t // group).wait()

            span = pl.ds(pl.multiple_of(t * LANES, LANES), LANES)
            acc = jnp.zeros((LANES, LANES), f32)
            for k in range(lane_tiles):
                lanes = slice(k * LANES, (k + 1) * LANES)
                value = g[m, span, lanes].astype(f32)
                square = value * value
                acc = acc + square
                colacc[m, :, lanes] = colacc[m, :, lanes] + jnp.sum(
                    square.reshape(LANES // 8, 8, LANES), axis=0
                )
            rslot[m, me, :, span] = jnp.sum(acc.T, axis=0, keepdims=True)

        cslot[m, my_row] = jnp.sum(colacc[m], axis=0, keepdims=True)

    def share(ref, axis, count, index, send_sem, recv_sem):
        for step in range(1, count):
            peer = lax.rem(index + step, count)
            pltpu.make_async_remote_copy(
                src_ref=ref.at[index],
                dst_ref=ref.at[index],
                send_sem=send_sem,
                recv_sem=recv_sem,
                device_id={axis: peer},
                device_id_type=MESH,
            ).start()

    def others(ref, axis, count, index, send_sem, recv_sem):
        return pltpu.make_async_remote_copy(
            src_ref=ref.at[pl.ds(0, count - 1)],
            dst_ref=ref.at[pl.ds(0, count - 1)],
            send_sem=send_sem,
            recv_sem=recv_sem,
            device_id={axis: lax.rem(index + 1, count)},
            device_id_type=MESH,
        )

    def gather(ref, axis, count, index, send_sem, recv_sem):
        others(ref, axis, count, index, send_sem, recv_sem).wait_recv()
        total = ref[0]
        for i in range(1, count):
            total = total + ref[i]
        return total

    def settle_shares(m):
        others(cslot.at[m], "row", rows, my_row, csend.at[m], crecv.at[m]).wait_send()
        others(rslot.at[m], "col", cols, me, rsend.at[m], rrecv.at[m]).wait_send()
        others(s1.at[m], "col", cols, me, s1send.at[m], s1recv.at[m]).wait_send()
        others(s2.at[m], "row", rows, my_row, s2send.at[m], s2recv.at[m]).wait_send()

    def share_factors(m):
        share(cslot.at[m], "row", rows, my_row, csend.at[m], crecv.at[m])
        share(rslot.at[m], "col", cols, me, rsend.at[m], rrecv.at[m])

    stats(0)
    pl.semaphore_wait(barrier, cols - 1 + rows - 1)
    share_factors(0)
    own_tokens.wait()
    for h in range(FIRST):
        token_send(h, (), bits[0])
    for h in range(PARTS):
        token_send(h, (), bits[-1])
    stats(1)
    share_factors(1)
    for h in range(FIRST, PARTS):
        token_send(h, (), bits[0])

    all_w.start()

    def lane_sum(value):
        total = value[:, :LANES]
        for t in range(1, tiles):
            total = total + value[:, t * LANES : (t + 1) * LANES]
        return total

    def norm_pass(m):
        col_total = gather(cslot.at[m], "row", rows, my_row, csend.at[m], crecv.at[m])
        col_new = decay_rate * cf_ref[pl.ds(m, 1), :] + (1.0 - decay_rate) * (
            col_total / hidden_units + tiny_eps
        )
        cnew[pl.ds(m, 1), :] = col_new
        cgain[m] = 1.0 / col_new

        @pl.loop(0, tiles)
        def _(t):
            span = pl.ds(pl.multiple_of(t * LANES, LANES), LANES)
            acc = jnp.zeros((LANES, LANES), f32)
            for k in range(lane_tiles):
                lanes = slice(k * LANES, (k + 1) * LANES)
                value = g[m, span, lanes].astype(f32)
                acc = acc + value * value * cgain[m, :, lanes]
            rnorm[pl.ds(m, 1), span] = jnp.sum(acc.T, axis=0, keepdims=True)

        row_total = gather(rslot.at[m], "col", cols, me, rsend.at[m], rrecv.at[m])
        row_new = decay_rate * rf_ref[pl.ds(m, 1), :] + (1.0 - decay_rate) * (
            row_total / features + tiny_eps
        )
        rnew[pl.ds(m, 1), :] = row_new
        s1[m, me] = jnp.zeros((8, LANES), f32)
        s1[m, me, 0:1, :] = lane_sum(rnorm[pl.ds(m, 1), :] / row_new)
        share(s1.at[m], "col", cols, me, s1send.at[m], s1recv.at[m])

    def row_gains(m):
        row_root = jnp.sqrt(1.0 / rnew[pl.ds(m, 1), :])
        for t in range(tiles):
            lanes = slice(t * LANES, (t + 1) * LANES)
            rcol[m, lanes, :] = jnp.broadcast_to(row_root[:, lanes], (LANES, LANES)).T

    def share_norm(m):
        s2[m, my_row] = jnp.zeros((8, LANES), f32)
        s2[m, my_row, 1:2, :] = lane_sum(rnew[pl.ds(m, 1), :])
        norm = gather(s1.at[m], "col", cols, me, s1send.at[m], s1recv.at[m])
        s2[m, my_row, 0:1, :] = norm[0:1, :]
        share(s2.at[m], "row", rows, my_row, s2send.at[m], s2recv.at[m])

    def set_rate(m):
        totals = gather(s2.at[m], "row", rows, my_row, s2send.at[m], s2recv.at[m])
        totals = jnp.sum(totals, axis=1, keepdims=True)
        row_mean = totals[1:2, :] / hidden_units
        mean_square = row_mean * totals[0:1, :] / (hidden_units * features)
        clip_scale = jnp.maximum(1.0, jnp.sqrt(mean_square) / clip_limit)
        rate = jnp.sqrt(row_mean) * (learn_rate / clip_scale)
        cgain[m] = jnp.sqrt(cgain[m]) * rate

    def pass_on(h):
        token_wait(h, (bits[0],))
        token_send(h, (bits[0],), bits[-1])

    norm_pass(0)
    norm_pass(1)
    row_copy = pltpu.make_async_copy(rnew, row_out, o_sem.at[0])
    row_copy.start()
    col_copy = pltpu.make_async_copy(cnew, col_out, o_sem.at[1])
    col_copy.start()
    share_norm(0)
    row_gains(0)
    row_gains(1)
    for h in range(PARTS):
        pass_on(h)
    share_norm(1)
    for masks in [(), (bits[0],)]:
        for h in range(PARTS):
            for mask in bits[1:-1]:
                token_send(h, masks, mask)
    all_w.wait()
    set_rate(0)
    early = [(), (bits[0],)]
    for h in range(PARTS):
        for before in early:
            token_wait(h, before + (bits[-1],))

    def late_tokens():
        for step in range(1, len(bits) - 1):
            for before in subsets(bits[:step]):
                for h in range(PARTS):
                    masks = before + (bits[step],)
                    token_wait(h, masks)
                    for mask in bits[step + 1 :]:
                        token_send(h, masks, mask)
        for before in subsets(bits[:-1]):
            if before not in early:
                for h in range(PARTS):
                    token_wait(h, before + (bits[-1],))

    defer = len(bits) == 3 and half == 2
    if not defer:
        late_tokens()

    def renew(c, m):
        @pl.loop(0, width // STRIP)
        def _(i):
            span = pl.ds(pl.multiple_of(c * width + i * STRIP, STRIP), STRIP)
            root = rcol[m, span, :]
            for k in range(lane_tiles):
                lanes = slice(k * LANES, (k + 1) * LANES)
                step = g[m, span, lanes].astype(f32) * root * cgain[m, :, lanes]
                w[m, span, lanes] = (w[m, span, lanes].astype(f32) - step).astype(jnp.bfloat16)

    def place(k):
        rest = lax.rem(k, 2 * chunks)
        return rest // 2, lax.rem(k, 2)

    def product(d, k):
        c, m = place(k)
        b = block_of(d, k)
        chosen = tok[pl.ds(pl.multiple_of(b * token_block, token_block), token_block), :]
        prod[...] = lax.dot_general(
            chosen,
            w[m, pl.ds(pl.multiple_of(c * width, width), width), :],
            (((1,), (1,)), ((), ())),
            preferred_element_type=f32,
        )

    def data_copy(d, k):
        return pltpu.make_async_remote_copy(
            src_ref=sbuf.at[d, k],
            dst_ref=rbuf.at[d, k],
            send_sem=dsend.at[d],
            recv_sem=drecv.at[d, k],
            device_id={"col": me + 2 * d - 1},
            device_id_type=MESH,
        )

    def peak_copy(d, k):
        return pltpu.make_async_remote_copy(
            src_ref=sscale.at[d, k],
            dst_ref=rscale.at[d, k],
            send_sem=psend.at[d],
            recv_sem=precv.at[d, k],
            device_id={"col": me + 2 * d - 1},
            device_id_type=MESH,
        )

    def add_received(d, k):
        peak_copy(d, k).wait_recv()
        data_copy(d, k).wait_recv()
        unit = rscale[d, k] / code_span

        @pl.loop(0, token_block // STRIP)
        def _(i):
            span = pl.ds(pl.multiple_of(i * STRIP, STRIP), STRIP)
            code = rbuf[d, k, span, :].astype(f32)
            value = (jnp.log2(jnp.abs(code)) + 0.5 * code_span) * unit
            prod[span, :] = prod[span, :] + jnp.where(code < 0, -value, value)

    def send_on(d, k):
        def strip_peak(i, peak):
            span = pl.ds(pl.multiple_of(i * STRIP, STRIP), STRIP)
            part = jnp.abs(prod[span, :])
            return jnp.maximum(peak, jnp.max(part.reshape(STRIP // 8, 8, width), axis=0))

        peak = lax.fori_loop(0, token_block // STRIP, strip_peak, jnp.zeros((8, width), f32))
        peak = jnp.maximum(jnp.max(peak, axis=0, keepdims=True), 1e-30)
        sscale[d, k] = peak
        peak_copy(d, k).start()
        unit = code_span / peak

        @pl.loop(0, token_block // STRIP)
        def _(i):
            span = pl.ds(pl.multiple_of(i * STRIP, STRIP), STRIP)
            part = prod[span, :]
            size = jnp.exp2(jnp.abs(part) * unit - 0.5 * code_span)
            sbuf[d, k, span, :] = jnp.where(part < 0, -size, size).astype(jnp.bfloat16)

        data_copy(d, k).start()

    def block_of(d, k):
        return d * half + lax.rem(k // (2 * chunks) + my_row // 2, half)

    def hidden_copy(k):
        c, _ = place(k)
        return pltpu.make_async_remote_copy(
            src_ref=hbuf.at[k // 2],
            dst_ref=out_ref.at[:, pl.ds(pl.multiple_of(c * width, width), width)],
            send_sem=hsend.at[k // (2 * chunks)],
            recv_sem=hrecv,
            device_id={"col": block_of(far, k)},
            device_id_type=MESH,
        )

    def local_copy(k):
        c, _ = place(k)
        return pltpu.make_async_copy(
            hbuf.at[k // 2],
            out_ref.at[:, pl.ds(pl.multiple_of(c * width, width), width)],
            lsend,
        )

    def finish(k):
        b = block_of(far, k)

        @pl.loop(0, token_block // STRIP)
        def _(i):
            span = pl.ds(pl.multiple_of(i * STRIP, STRIP), STRIP)
            gate = kept[span, :]
            value = (gate / (1.0 + jnp.exp(-gate)) * prod[span, :]).astype(jnp.bfloat16)
            hbuf[k // 2, span, :] = value

        @pl.when(b == me)
        def _():
            local_copy(k).start()

        @pl.when(b != me)
        def _():
            hidden_copy(k).start()

    near = 1 - me // half
    far = 1 - near
    depth = near * me + far * (cols - 1 - me)
    inner = (depth + half - 1) // half
    lag = items + inner * (INNER_LAG - items)

    @pl.loop(0, 2 * items)
    def _(k):
        @pl.when(k < items)
        def _():
            c, m = place(k)
            pl.when(k == 1)(functools.partial(set_rate, 1))
            if defer:
                pl.when(k == 2 * chunks - 1)(late_tokens)

            @pl.when(k < 2 * chunks)
            def _():
                renew(c, m)

            product(near, k)

            @pl.when(depth > 0)
            def _():
                add_received(near, k)

            send_on(near, k)

        @pl.when((k >= lag) & (k < items + lag))
        def _():
            j = k - lag
            product(far, j)
            add_received(far, j)

            @pl.when(depth > 0)
            def _():
                send_on(far, j)

            @pl.when((depth == 0) & (lax.rem(j, 2) == 0))
            def _():
                kept[...] = prod[...]

            @pl.when((depth == 0) & (lax.rem(j, 2) == 1))
            def _():
                finish(j)

    def sent(ref, sem):
        pltpu.make_async_remote_copy(
            src_ref=ref,
            dst_ref=ref,
            send_sem=sem,
            recv_sem=hrecv,
            device_id={"col": lax.rem(me + 1, cols)},
            device_id_type=MESH,
        ).wait_send()

    for m in range(2):
        settle_shares(m)
    sent(tok.at[pl.ds(0, (rows - 1) * local_tokens), :], tsend)
    row_copy.wait()
    col_copy.wait()
    sent(sbuf.at[near], dsend.at[near])
    sent(sscale.at[near], psend.at[near])

    @pl.when(depth > 0)
    def _():
        sent(sbuf.at[far], dsend.at[far])
        sent(sscale.at[far], psend.at[far])

    @pl.when(depth == 0)
    def _():
        for turn in range(half):
            @pl.when(block_of(far, 2 * chunks * turn) != me)
            def _():
                sent(hbuf.at[pl.ds(turn * chunks, chunks)], hsend.at[turn])

        pltpu.make_async_copy(out_ref, out_ref, lsend).wait()

    @pl.when(depth > 0)
    def _():
        pltpu.make_async_remote_copy(
            src_ref=out_ref,
            dst_ref=out_ref,
            send_sem=hsend.at[0],
            recv_sem=hrecv,
            device_id={"col": lax.rem(me + 1, cols)},
            device_id_type=MESH,
        ).wait_recv()


def settle(h_in, r_in, c_in, h_out, r_out, c_out, h_buf, r_buf, c_buf, sems):
    pieces = 4
    depth = h_in.shape[0] // pieces
    moves = [(r_in, r_buf, r_out), (c_in, c_buf, c_out)]
    for i in range(pieces):
        span = pl.ds(i * depth, depth)
        moves.append((h_in.at[span, :], h_buf.at[span, :], h_out.at[span, :]))
    loads = [
        pltpu.make_async_copy(a, b, sems.at[0, i]) for i, (a, b, _) in enumerate(moves)
    ]
    stores = [
        pltpu.make_async_copy(b, c, sems.at[1, i]) for i, (_, b, c) in enumerate(moves)
    ]
    for load in loads:
        load.start()
    for load, store in zip(loads, stores):
        load.wait()
        store.start()
    for store in stores:
        store.wait()


def local(rows, cols, tokens, weights, gradients, row_factors, col_factors):
    row_block, col_block = gradients.shape[1], gradients.shape[2]
    all_tokens = tokens.shape[0] * rows
    token_block = all_tokens // cols
    chunks = max(n for n in (1, 2, 3, 4, 5, 6, 7) if row_block % (n * LANES) == 0)
    width = row_block // chunks
    items = 2 * chunks * (cols // 2)
    tiles = row_block // LANES
    f32, bf16 = jnp.float32, jnp.bfloat16
    vmem = pl.BlockSpec(memory_space=pltpu.VMEM)
    anywhere = pl.BlockSpec(memory_space=pl.ANY)
    dma = pltpu.SemaphoreType.DMA
    shapes = (
        jax.ShapeDtypeStruct((token_block, row_block), bf16),
        jax.ShapeDtypeStruct((2, row_block), f32),
        jax.ShapeDtypeStruct((2, col_block), f32),
    )
    results = pl.pallas_call(
        functools.partial(body, rows, cols, chunks),
        out_shape=shapes,
        in_specs=[anywhere, anywhere, anywhere, vmem, vmem],
        out_specs=(anywhere, anywhere, anywhere),
        scratch_shapes=[
            pltpu.VMEM((all_tokens, col_block), bf16),
            pltpu.VMEM((2, row_block, col_block), bf16),
            pltpu.VMEM((2, row_block, col_block), bf16),
            pltpu.VMEM((2, row_block, LANES), f32),
            pltpu.VMEM((2, 8, col_block), f32),
            pltpu.VMEM((2, 1, col_block), f32),
            pltpu.VMEM((2, row_block), f32),
            pltpu.VMEM((2, col_block), f32),
            pltpu.VMEM((2, row_block), f32),
            pltpu.VMEM((2, cols, 1, row_block), f32),
            pltpu.VMEM((2, rows, 1, col_block), f32),
            pltpu.VMEM((2, cols, 8, LANES), f32),
            pltpu.VMEM((2, rows, 8, LANES), f32),
            pltpu.VMEM((token_block, width), f32),
            pltpu.VMEM((token_block, width), f32),
            pltpu.VMEM((2, items, token_block, width), bf16),
            pltpu.VMEM((2, items, token_block, width), bf16),
            pltpu.VMEM((2, items, 1, width), f32),
            pltpu.VMEM((2, items, 1, width), f32),
            pltpu.VMEM((items // 2, token_block, width), bf16),
            dma((2,)),
            dma,
            dma((tiles // (2 if tiles % 2 == 0 else 1) + 1,)),
            dma,
            dma,
            dma,
            dma((PARTS, rows)),
            dma((2,)),
            dma((2,)),
            dma((2,)),
            dma((2,)),
            dma((2,)),
            dma((2,)),
            dma((2,)),
            dma((2,)),
            dma((2,)),
            dma((2, items)),
            dma((2,)),
            dma((2, items)),
            dma((cols // 2,)),
            dma,
        ],
        compiler_params=pltpu.CompilerParams(
            collective_id=0, has_side_effects=True, vmem_limit_bytes=67000000
        ),
    )(tokens, weights, gradients, row_factors, col_factors)
    return pl.pallas_call(
        settle,
        out_shape=shapes,
        in_specs=[anywhere, anywhere, anywhere],
        out_specs=(anywhere, anywhere, anywhere),
        scratch_shapes=[
            pltpu.VMEM((token_block, row_block), bf16),
            pltpu.VMEM((2, row_block), f32),
            pltpu.VMEM((2, col_block), f32),
            dma((2, 6)),
        ],
    )(*results)


def solution(mesh):
    placed = (
        P("row", "col"),
        P(None, "row", "col"),
        P(None, "row", "col"),
        P(None, "row"),
        P(None, "col"),
    )
    return jax.shard_map(
        functools.partial(local, mesh.shape["row"], mesh.shape["col"]),
        mesh=mesh,
        in_specs=placed,
        out_specs=(P("col", "row"), P(None, "row"), P(None, "col")),
        check_vma=False,
    )
```

```python
import functools
import jax
import jax.numpy as jnp
from jax import lax
from jax.experimental import pallas as pl
from jax.experimental.pallas import tpu as pltpu
from jax.sharding import PartitionSpec as P

decay_rate = 0.5
learn_rate = 0.01
clip_limit = 1.0
tiny_eps = 1e-30
code_span = 250.0


MESH = pl.DeviceIdType.MESH
LANES = 128
STRIP = 32
INNER_LAG = 2
CUTS = ((0, 3), (3, 3), (6, 2))
PARTS = len(CUTS)
FIRST = 1


def flip(value, mask):
    return value + mask * (1 - 2 * ((value // mask) % 2))


def flips(value, masks):
    for mask in masks:
        value = flip(value, mask)
    return value


def subsets(masks):
    out = [()]
    for mask in masks:
        out = out + [item + (mask,) for item in out]
    return out


def body(
    rows,
    cols,
    chunks,
    tok_in,
    w_in,
    g_in,
    rf_ref,
    cf_ref,
    out_ref,
    row_out,
    col_out,
    tok,
    w,
    g,
    rcol,
    colacc,
    cgain,
    rnew,
    cnew,
    rnorm,
    rslot,
    cslot,
    s1,
    s2,
    prod,
    kept,
    sbuf,
    rbuf,
    sscale,
    rscale,
    hbuf,
    o_sem,
    lsend,
    g_sem,
    w_sem,
    t_sem,
    tsend,
    trecv,
    rsend,
    rrecv,
    csend,
    crecv,
    s1send,
    s1recv,
    s2send,
    s2recv,
    dsend,
    drecv,
    psend,
    precv,
    hsend,
    hrecv,
):
    f32 = jnp.float32
    my_row = lax.axis_index("row")
    me = lax.axis_index("col")
    row_block, col_block = g.shape[1], g.shape[2]
    hidden_units, features = row_block * rows, col_block * cols
    tiles = row_block // LANES
    lane_tiles = col_block // LANES
    local_tokens = tok_in.shape[0]
    token_block = local_tokens * rows // cols
    width = row_block // chunks
    half = cols // 2
    items = 2 * chunks * half

    barrier = pltpu.get_barrier_semaphore()
    for step in range(1, cols):
        pl.semaphore_signal(
            barrier, inc=1, device_id={"col": lax.rem(me + step, cols)}, device_id_type=MESH
        )
    for step in range(1, rows):
        pl.semaphore_signal(
            barrier, inc=1, device_id={"row": lax.rem(my_row + step, rows)}, device_id_type=MESH
        )

    group = 2 if tiles % 2 == 0 else 1

    def g_copy(t):
        span = pl.ds(t * LANES, LANES)
        return pltpu.make_async_copy(g_in.at[0, span, :], g.at[0, span, :], g_sem.at[t])

    def later_g(t):
        span = pl.ds(t * LANES * group, LANES * group)
        return pltpu.make_async_copy(
            g_in.at[1, span, :], g.at[1, span, :], g_sem.at[tiles + t]
        )

    all_w = pltpu.make_async_copy(w_in, w, w_sem)

    own_tokens = pltpu.make_async_copy(
        tok_in, tok.at[pl.ds(my_row * local_tokens, local_tokens), :], t_sem
    )
    own_tokens.start()

    @pl.loop(0, tiles)
    def _(t):
        g_copy(t).start()

    @pl.loop(0, tiles // group)
    def _(t):
        later_g(t).start()


    bits = [1 << i for i in reversed(range(rows.bit_length() - 1))]
    eighth = local_tokens // 8

    def token_copy(h, masks, mask):
        block = flips(my_row, masks)
        first, size = CUTS[h]
        part = tok.at[pl.ds(block * local_tokens + first * eighth, size * eighth), :]
        return pltpu.make_async_remote_copy(
            src_ref=part,
            dst_ref=part,
            send_sem=tsend,
            recv_sem=trecv.at[h, block],
            device_id={"row": flip(my_row, mask)},
            device_id_type=MESH,
        )

    def token_send(h, masks, mask):
        token_copy(h, masks, mask).start()

    def token_wait(h, masks):
        token_copy(h, masks, masks[-1]).wait_recv()

    def stats(m):
        colacc[m] = jnp.zeros((8, col_block), f32)

        @pl.loop(0, tiles)
        def _(t):
            if m == 0:
                g_copy(t).wait()
            else:
                @pl.when(lax.rem(t, group) == 0)
                def _():
                    later_g(t // group).wait()

            span = pl.ds(pl.multiple_of(t * LANES, LANES), LANES)
            acc = jnp.zeros((LANES, LANES), f32)
            for k in range(lane_tiles):
                lanes = slice(k * LANES, (k + 1) * LANES)
                value = g[m, span, lanes].astype(f32)
                square = value * value
                acc = acc + square
                colacc[m, :, lanes] = colacc[m, :, lanes] + jnp.sum(
                    square.reshape(LANES // 8, 8, LANES), axis=0
                )
            rslot[m, me, :, span] = jnp.sum(acc.T, axis=0, keepdims=True)

        cslot[m, my_row] = jnp.sum(colacc[m], axis=0, keepdims=True)

    def share(ref, axis, count, index, send_sem, recv_sem):
        for step in range(1, count):
            peer = lax.rem(index + step, count)
            pltpu.make_async_remote_copy(
                src_ref=ref.at[index],
                dst_ref=ref.at[index],
                send_sem=send_sem,
                recv_sem=recv_sem,
                device_id={axis: peer},
                device_id_type=MESH,
            ).start()

    def others(ref, axis, count, index, send_sem, recv_sem):
        return pltpu.make_async_remote_copy(
            src_ref=ref.at[pl.ds(0, count - 1)],
            dst_ref=ref.at[pl.ds(0, count - 1)],
            send_sem=send_sem,
            recv_sem=recv_sem,
            device_id={axis: lax.rem(index + 1, count)},
            device_id_type=MESH,
        )

    def gather(ref, axis, count, index, send_sem, recv_sem):
        others(ref, axis, count, index, send_sem, recv_sem).wait_recv()
        total = ref[0]
        for i in range(1, count):
            total = total + ref[i]
        return total

    def settle_shares(m):
        others(cslot.at[m], "row", rows, my_row, csend.at[m], crecv.at[m]).wait_send()
        others(rslot.at[m], "col", cols, me, rsend.at[m], rrecv.at[m]).wait_send()
        others(s1.at[m], "col", cols, me, s1send.at[m], s1recv.at[m]).wait_send()
        others(s2.at[m], "row", rows, my_row, s2send.at[m], s2recv.at[m]).wait_send()

    def share_factors(m):
        share(cslot.at[m], "row", rows, my_row, csend.at[m], crecv.at[m])
        share(rslot.at[m], "col", cols, me, rsend.at[m], rrecv.at[m])

    stats(0)
    pl.semaphore_wait(barrier, cols - 1 + rows - 1)
    share_factors(0)
    own_tokens.wait()
    for h in range(FIRST):
        token_send(h, (), bits[0])
    for h in range(PARTS):
        token_send(h, (), bits[-1])
    stats(1)
    share_factors(1)
    for h in range(FIRST, PARTS):
        token_send(h, (), bits[0])

    all_w.start()

    def lane_sum(value):
        total = value[:, :LANES]
        for t in range(1, tiles):
            total = total + value[:, t * LANES : (t + 1) * LANES]
        return total

    def norm_pass(m):
        col_total = gather(cslot.at[m], "row", rows, my_row, csend.at[m], crecv.at[m])
        col_new = decay_rate * cf_ref[pl.ds(m, 1), :] + (1.0 - decay_rate) * (
            col_total / hidden_units + tiny_eps
        )
        cnew[pl.ds(m, 1), :] = col_new
        cgain[m] = 1.0 / col_new

        @pl.loop(0, tiles)
        def _(t):
            span = pl.ds(pl.multiple_of(t * LANES, LANES), LANES)
            acc = jnp.zeros((LANES, LANES), f32)
            for k in range(lane_tiles):
                lanes = slice(k * LANES, (k + 1) * LANES)
                value = g[m, span, lanes].astype(f32)
                acc = acc + value * value * cgain[m, :, lanes]
            rnorm[pl.ds(m, 1), span] = jnp.sum(acc.T, axis=0, keepdims=True)

        row_total = gather(rslot.at[m], "col", cols, me, rsend.at[m], rrecv.at[m])
        row_new = decay_rate * rf_ref[pl.ds(m, 1), :] + (1.0 - decay_rate) * (
            row_total / features + tiny_eps
        )
        rnew[pl.ds(m, 1), :] = row_new
        s1[m, me] = jnp.zeros((8, LANES), f32)
        s1[m, me, 0:1, :] = lane_sum(rnorm[pl.ds(m, 1), :] / row_new)
        share(s1.at[m], "col", cols, me, s1send.at[m], s1recv.at[m])

    def row_gains(m):
        row_root = jnp.sqrt(1.0 / rnew[pl.ds(m, 1), :])
        for t in range(tiles):
            lanes = slice(t * LANES, (t + 1) * LANES)
            rcol[m, lanes, :] = jnp.broadcast_to(row_root[:, lanes], (LANES, LANES)).T

    def share_norm(m):
        s2[m, my_row] = jnp.zeros((8, LANES), f32)
        s2[m, my_row, 1:2, :] = lane_sum(rnew[pl.ds(m, 1), :])
        norm = gather(s1.at[m], "col", cols, me, s1send.at[m], s1recv.at[m])
        s2[m, my_row, 0:1, :] = norm[0:1, :]
        share(s2.at[m], "row", rows, my_row, s2send.at[m], s2recv.at[m])

    def set_rate(m):
        totals = gather(s2.at[m], "row", rows, my_row, s2send.at[m], s2recv.at[m])
        totals = jnp.sum(totals, axis=1, keepdims=True)
        row_mean = totals[1:2, :] / hidden_units
        mean_square = row_mean * totals[0:1, :] / (hidden_units * features)
        clip_scale = jnp.maximum(1.0, jnp.sqrt(mean_square) / clip_limit)
        rate = jnp.sqrt(row_mean) * (learn_rate / clip_scale)
        cgain[m] = jnp.sqrt(cgain[m]) * rate

    def pass_on(h):
        token_wait(h, (bits[0],))
        token_send(h, (bits[0],), bits[-1])

    norm_pass(0)
    norm_pass(1)
    row_copy = pltpu.make_async_copy(rnew, row_out, o_sem.at[0])
    row_copy.start()
    col_copy = pltpu.make_async_copy(cnew, col_out, o_sem.at[1])
    col_copy.start()
    share_norm(0)
    row_gains(0)
    row_gains(1)
    for h in range(PARTS):
        pass_on(h)
    def spread_tokens():
        for masks in [(), (bits[0],)]:
            for h in range(PARTS):
                for mask in bits[1:-1]:
                    token_send(h, masks, mask)

    all_w.wait()
    set_rate(0)
    early = [(), (bits[0],)]
    for h in range(PARTS):
        for before in early:
            token_wait(h, before + (bits[-1],))

    def late_tokens():
        for step in range(1, len(bits) - 1):
            for before in subsets(bits[:step]):
                for h in range(PARTS):
                    masks = before + (bits[step],)
                    token_wait(h, masks)
                    for mask in bits[step + 1 :]:
                        token_send(h, masks, mask)
        for before in subsets(bits[:-1]):
            if before not in early:
                for h in range(PARTS):
                    token_wait(h, before + (bits[-1],))

    defer = len(bits) == 3 and half == 2
    if not defer:
        spread_tokens()
        late_tokens()

    def renew(c, m):
        @pl.loop(0, width // STRIP)
        def _(i):
            span = pl.ds(pl.multiple_of(c * width + i * STRIP, STRIP), STRIP)
            root = rcol[m, span, :]
            for k in range(lane_tiles):
                lanes = slice(k * LANES, (k + 1) * LANES)
                step = g[m, span, lanes].astype(f32) * root * cgain[m, :, lanes]
                w[m, span, lanes] = (w[m, span, lanes].astype(f32) - step).astype(jnp.bfloat16)

    def place(k):
        rest = lax.rem(k, 2 * chunks)
        late = (rest // 4 + 3) // 4 if chunks > 1 else 1
        c = late * (rest // 2) + (1 - late) * lax.rem(rest, 2)
        m = late * lax.rem(rest, 2) + (1 - late) * (rest // 2)
        return c, m

    def result_slot(k):
        return k // (2 * chunks) * chunks + place(k)[0]

    def product(d, k):
        c, m = place(k)
        b = block_of(d, k)
        chosen = tok[pl.ds(pl.multiple_of(b * token_block, token_block), token_block), :]
        prod[...] = lax.dot_general(
            chosen,
            w[m, pl.ds(pl.multiple_of(c * width, width), width), :],
            (((1,), (1,)), ((), ())),
            preferred_element_type=f32,
        )

    def data_copy(d, k):
        return pltpu.make_async_remote_copy(
            src_ref=sbuf.at[d, k],
            dst_ref=rbuf.at[d, k],
            send_sem=dsend.at[d],
            recv_sem=drecv.at[d, k],
            device_id={"col": me + 2 * d - 1},
            device_id_type=MESH,
        )

    def peak_copy(d, k):
        return pltpu.make_async_remote_copy(
            src_ref=sscale.at[d, k],
            dst_ref=rscale.at[d, k],
            send_sem=psend.at[d],
            recv_sem=precv.at[d, k],
            device_id={"col": me + 2 * d - 1},
            device_id_type=MESH,
        )

    def add_received(d, k):
        peak_copy(d, k).wait_recv()
        data_copy(d, k).wait_recv()
        unit = rscale[d, k] / code_span

        @pl.loop(0, token_block // STRIP)
        def _(i):
            span = pl.ds(pl.multiple_of(i * STRIP, STRIP), STRIP)
            code = rbuf[d, k, span, :].astype(f32)
            value = (jnp.log2(jnp.abs(code)) + 0.5 * code_span) * unit
            prod[span, :] = prod[span, :] + jnp.where(code < 0, -value, value)

    def send_on(d, k):
        def strip_peak(i, peak):
            span = pl.ds(pl.multiple_of(i * STRIP, STRIP), STRIP)
            part = jnp.abs(prod[span, :])
            return jnp.maximum(peak, jnp.max(part.reshape(STRIP // 8, 8, width), axis=0))

        peak = lax.fori_loop(0, token_block // STRIP, strip_peak, jnp.zeros((8, width), f32))
        peak = jnp.maximum(jnp.max(peak, axis=0, keepdims=True), 1e-30)
        sscale[d, k] = peak
        peak_copy(d, k).start()
        unit = code_span / peak

        @pl.loop(0, token_block // STRIP)
        def _(i):
            span = pl.ds(pl.multiple_of(i * STRIP, STRIP), STRIP)
            part = prod[span, :]
            size = jnp.exp2(jnp.abs(part) * unit - 0.5 * code_span)
            sbuf[d, k, span, :] = jnp.where(part < 0, -size, size).astype(jnp.bfloat16)

        data_copy(d, k).start()

    def block_of(d, k):
        return d * half + lax.rem(k // (2 * chunks) + my_row // 2, half)

    def hidden_copy(k):
        c, _ = place(k)
        return pltpu.make_async_remote_copy(
            src_ref=hbuf.at[result_slot(k)],
            dst_ref=out_ref.at[:, pl.ds(pl.multiple_of(c * width, width), width)],
            send_sem=hsend.at[k // (2 * chunks)],
            recv_sem=hrecv,
            device_id={"col": block_of(far, k)},
            device_id_type=MESH,
        )

    def local_copy(k):
        c, _ = place(k)
        return pltpu.make_async_copy(
            hbuf.at[result_slot(k)],
            out_ref.at[:, pl.ds(pl.multiple_of(c * width, width), width)],
            lsend,
        )

    def finish(k):
        b = block_of(far, k)
        c = lax.rem(place(k)[0], 2)
        slot = result_slot(k)

        @pl.loop(0, token_block // STRIP)
        def _(i):
            span = pl.ds(pl.multiple_of(i * STRIP, STRIP), STRIP)
            gate = kept[c, span, :]
            value = (gate / (1.0 + jnp.exp(-gate)) * prod[span, :]).astype(jnp.bfloat16)
            hbuf[slot, span, :] = value

        @pl.when(b == me)
        def _():
            local_copy(k).start()

        @pl.when(b != me)
        def _():
            hidden_copy(k).start()

    near = 1 - me // half
    far = 1 - near
    depth = near * me + far * (cols - 1 - me)
    inner = (depth + half - 1) // half
    lead = 2 if chunks > 1 else 1
    lag = items + inner * (INNER_LAG - items)

    @pl.loop(0, 2 * items)
    def _(k):
        @pl.when(k < items)
        def _():
            c, m = place(k)
            @pl.when(k == 1)
            def _():
                share_norm(1)
                if defer:
                    spread_tokens()

            pl.when(k == lead)(functools.partial(set_rate, 1))
            if defer:
                pl.when(k == 2 * chunks - 1)(late_tokens)

            @pl.when(k < 2 * chunks)
            def _():
                renew(c, m)

            product(near, k)

            @pl.when(depth > 0)
            def _():
                add_received(near, k)

            send_on(near, k)

        @pl.when((k >= lag) & (k < items + lag))
        def _():
            j = k - lag
            product(far, j)
            add_received(far, j)

            @pl.when(depth > 0)
            def _():
                send_on(far, j)

            far_c, far_m = place(j)

            @pl.when((depth == 0) & (far_m == 0))
            def _():
                kept[lax.rem(far_c, 2)] = prod[...]

            @pl.when((depth == 0) & (far_m == 1))
            def _():
                finish(j)

    def sent(ref, sem):
        pltpu.make_async_remote_copy(
            src_ref=ref,
            dst_ref=ref,
            send_sem=sem,
            recv_sem=hrecv,
            device_id={"col": lax.rem(me + 1, cols)},
            device_id_type=MESH,
        ).wait_send()

    for m in range(2):
        settle_shares(m)
    sent(tok.at[pl.ds(0, (rows - 1) * local_tokens), :], tsend)
    row_copy.wait()
    col_copy.wait()
    sent(sbuf.at[near], dsend.at[near])
    sent(sscale.at[near], psend.at[near])

    @pl.when(depth > 0)
    def _():
        sent(sbuf.at[far], dsend.at[far])
        sent(sscale.at[far], psend.at[far])

    @pl.when(depth == 0)
    def _():
        for turn in range(half):
            @pl.when(block_of(far, 2 * chunks * turn) != me)
            def _():
                sent(hbuf.at[pl.ds(turn * chunks, chunks)], hsend.at[turn])

        pltpu.make_async_copy(out_ref, out_ref, lsend).wait()

    @pl.when(depth > 0)
    def _():
        pltpu.make_async_remote_copy(
            src_ref=out_ref,
            dst_ref=out_ref,
            send_sem=hsend.at[0],
            recv_sem=hrecv,
            device_id={"col": lax.rem(me + 1, cols)},
            device_id_type=MESH,
        ).wait_recv()


def settle(h_in, r_in, c_in, h_out, r_out, c_out, h_buf, r_buf, c_buf, sems):
    pieces = 4
    depth = h_in.shape[0] // pieces
    moves = [(r_in, r_buf, r_out), (c_in, c_buf, c_out)]
    for i in range(pieces):
        span = pl.ds(i * depth, depth)
        moves.append((h_in.at[span, :], h_buf.at[span, :], h_out.at[span, :]))
    loads = [
        pltpu.make_async_copy(a, b, sems.at[0, i]) for i, (a, b, _) in enumerate(moves)
    ]
    stores = [
        pltpu.make_async_copy(b, c, sems.at[1, i]) for i, (_, b, c) in enumerate(moves)
    ]
    for load in loads:
        load.start()
    for load, store in zip(loads, stores):
        load.wait()
        store.start()
    for store in stores:
        store.wait()


def local(rows, cols, tokens, weights, gradients, row_factors, col_factors):
    row_block, col_block = gradients.shape[1], gradients.shape[2]
    all_tokens = tokens.shape[0] * rows
    token_block = all_tokens // cols
    chunks = max(n for n in (1, 2, 3, 4, 5, 6, 7) if row_block % (n * LANES) == 0)
    width = row_block // chunks
    items = 2 * chunks * (cols // 2)
    tiles = row_block // LANES
    f32, bf16 = jnp.float32, jnp.bfloat16
    vmem = pl.BlockSpec(memory_space=pltpu.VMEM)
    anywhere = pl.BlockSpec(memory_space=pl.ANY)
    dma = pltpu.SemaphoreType.DMA
    shapes = (
        jax.ShapeDtypeStruct((token_block, row_block), bf16),
        jax.ShapeDtypeStruct((2, row_block), f32),
        jax.ShapeDtypeStruct((2, col_block), f32),
    )
    results = pl.pallas_call(
        functools.partial(body, rows, cols, chunks),
        out_shape=shapes,
        in_specs=[anywhere, anywhere, anywhere, vmem, vmem],
        out_specs=(anywhere, anywhere, anywhere),
        scratch_shapes=[
            pltpu.VMEM((all_tokens, col_block), bf16),
            pltpu.VMEM((2, row_block, col_block), bf16),
            pltpu.VMEM((2, row_block, col_block), bf16),
            pltpu.VMEM((2, row_block, LANES), f32),
            pltpu.VMEM((2, 8, col_block), f32),
            pltpu.VMEM((2, 1, col_block), f32),
            pltpu.VMEM((2, row_block), f32),
            pltpu.VMEM((2, col_block), f32),
            pltpu.VMEM((2, row_block), f32),
            pltpu.VMEM((2, cols, 1, row_block), f32),
            pltpu.VMEM((2, rows, 1, col_block), f32),
            pltpu.VMEM((2, cols, 8, LANES), f32),
            pltpu.VMEM((2, rows, 8, LANES), f32),
            pltpu.VMEM((token_block, width), f32),
            pltpu.VMEM((2, token_block, width), f32),
            pltpu.VMEM((2, items, token_block, width), bf16),
            pltpu.VMEM((2, items, token_block, width), bf16),
            pltpu.VMEM((2, items, 1, width), f32),
            pltpu.VMEM((2, items, 1, width), f32),
            pltpu.VMEM((items // 2, token_block, width), bf16),
            dma((2,)),
            dma,
            dma((2 * tiles // (1 if tiles % 2 else 2) + (0 if tiles % 2 else tiles // 2),)),
            dma,
            dma,
            dma,
            dma((PARTS, rows)),
            dma((2,)),
            dma((2,)),
            dma((2,)),
            dma((2,)),
            dma((2,)),
            dma((2,)),
            dma((2,)),
            dma((2,)),
            dma((2,)),
            dma((2, items)),
            dma((2,)),
            dma((2, items)),
            dma((cols // 2,)),
            dma,
        ],
        compiler_params=pltpu.CompilerParams(
            collective_id=0, has_side_effects=True, vmem_limit_bytes=67000000
        ),
    )(tokens, weights, gradients, row_factors, col_factors)
    return pl.pallas_call(
        settle,
        out_shape=shapes,
        in_specs=[anywhere, anywhere, anywhere],
        out_specs=(anywhere, anywhere, anywhere),
        scratch_shapes=[
            pltpu.VMEM((token_block, row_block), bf16),
            pltpu.VMEM((2, row_block), f32),
            pltpu.VMEM((2, col_block), f32),
            dma((2, 6)),
        ],
    )(*results)


def solution(mesh):
    placed = (
        P("row", "col"),
        P(None, "row", "col"),
        P(None, "row", "col"),
        P(None, "row"),
        P(None, "col"),
    )
    return jax.shard_map(
        functools.partial(local, mesh.shape["row"], mesh.shape["col"]),
        mesh=mesh,
        in_specs=placed,
        out_specs=(P("col", "row"), P(None, "row"), P(None, "col")),
        check_vma=False,
    )
```
